32 devices in a mesh: scen: 16 (over z, y, x), fac: 2 (over core).
Axes of the slice: x: 2, y: 2, z: 4, core: 2. Of those that a mesh axis runs over, the one named last changes fastest.
Arguments:
- scenario_pnl: float32 [16384, 2048], P('scen', 'fac'), may hold values from -300 to 300
Outputs:
- covariance: float32 [2048, 2048], P('scen', 'fac')
- factor_means: float32 [2048], P('fac')
The draws below stay inside these ranges and needn't reach their ends.
All inputs are finite; a program needn't handle non-finite values.
Results may differ from the reference program's by a relative error of at most 0.0003.
Values sent between devices are 32-bit elements; how exact they have to be, the bound alone decides.
A program may use at most 64 MiB of HBM per device.

```python
import jax
import jax.numpy as jnp
from jax import lax

F = 2048
SCENARIOS = 16384


def draw_scenario_pnl(key, part):
    keys = jax.random.split(jax.random.fold_in(key, 11), 9)
    noise = jnp.clip(jax.random.normal(keys[0], (SCENARIOS, F), jnp.float32), -4.0, 4.0)
    first = jax.random.permutation(keys[1], F)
    second = jax.random.permutation(keys[2], F)
    mixed = noise + 0.5 * noise[:, first] + 0.5 * noise[:, second]
    levels = jnp.clip(0.8 * jax.random.normal(keys[3], (F,), jnp.float32), -2.0, 2.0)
    scales = jnp.exp(jax.random.uniform(keys[4], (F,), jnp.float32, jnp.log(0.4), jnp.log(2.5)))
    drift = 0.5 + jnp.arange(SCENARIOS, dtype=jnp.float32) / SCENARIOS
    drawn = scales[None, :] * (mixed + drift[:, None] * levels[None, :])
    chosen = jax.random.permutation(keys[6], F) < F // 8
    signs = jnp.where(jax.random.uniform(keys[7], (F,), jnp.float32) < 0.5, -1.0, 1.0)
    offsets = signs * jax.random.uniform(keys[8], (F,), jnp.float32, 200.0, 260.0)
    shifted = offsets[None, :] + mixed + 2.0 * (drift[:, None] - 1.0)
    return jnp.where(chosen[None, :], shifted, drawn)


def setup_inputs(seed: int = 0) -> dict:
    key_of = jax.random.split(jax.random.key(seed), 2)
    return {
        "scenario_pnl": draw_scenario_pnl(jax.random.fold_in(key_of[1], 71), 0),
    }


def reference(scenario_pnl):
    count = scenario_pnl.shape[0]
    factor_means = jnp.sum(scenario_pnl, axis=0) / count
    centered = scenario_pnl - factor_means[None, :]
    product = lax.dot_general(centered, centered, (((0,), (0,)), ((), ())), precision=lax.Precision.HIGHEST, preferred_element_type=jnp.float32)
    covariance = product / (count - 1)
    return covariance, factor_means
```

```python
import functools

import jax
import jax.numpy as jnp
from jax import lax
from jax.experimental import pallas as pl
from jax.experimental.pallas import tpu as pltpu
from jax.sharding import PartitionSpec as P

MESH = pl.DeviceIdType.MESH
LOADS = 4
TILE = 64


def block_gram(left, right):
    return lax.dot_general(
        left,
        right,
        (((0,), (0,)), ((), ())),
        precision=lax.Precision.HIGHEST,
        preferred_element_type=jnp.float32,
    )


def on_device(scenario_pnl):
    rows_here = scenario_pnl.shape[0]
    total_rows = rows_here * lax.axis_size("scen")
    local_sums = jnp.sum(scenario_pnl, axis=0)
    total_sums = lax.psum(local_sums, "scen")
    factor_means = total_sums / total_rows
    local_means = local_sums / rows_here
    data = scenario_pnl - local_means[None, :]
    partial_value = block_gram(lax.all_gather(data, "fac", axis=1, tiled=True), data)
    owned = lax.psum_scatter(partial_value, "scen", scatter_dimension=0, tiled=True)
    gathered = lax.all_gather(local_means, ("scen", "fac"), axis=0, tiled=True)
    spread_rows = gathered.reshape(lax.axis_size("scen"), -1)
    deviations = spread_rows - jnp.mean(spread_rows, axis=0, keepdims=True)
    owned_rows = owned.shape[0]
    column_width = owned.shape[1]
    row_part = lax.dynamic_slice_in_dim(
        deviations, lax.axis_index("scen") * owned_rows, owned_rows, 1
    )
    column_part = lax.dynamic_slice_in_dim(
        deviations, lax.axis_index("fac") * column_width, column_width, 1
    )
    owned = owned + rows_here * block_gram(row_part, column_part)
    covariance = owned / (total_rows - 1)
    return (covariance, factor_means)


def kernel(
    n, x_hbm, cov_ref, mean_ref,
    x_vm, other, hi_w, lo_w, hi_o, lo_o,
    send1, keep1, recv1, send2, keep2, recv2, zsend, zrecv,
    turned, landed, sums_own, sums_oth, dev_w, dev_o,
    load_sem, pair_s, pair_r, s1_s, s1_r, s2_s, s2_r, z_s, z_r, t_s, t_r,
    m_s, m_r, mo_s, mo_r,
):
    rows, width = x_hbm.shape
    half = n // 2
    block = width // half
    near, far = half // 2 + 1, half // 2
    depth = n // 4
    zh = depth // 2
    total_rows = rows * n

    s = lax.axis_index("scen")
    c = lax.axis_index("fac")
    z, y, x = s // 4, (s // 2) % 2, s % 2
    first = x * (1 - c) + y * c
    second = y * (1 - c) + x * c
    peer1 = s + (1 - 2 * x) * (1 - c) + (2 - 4 * y) * c
    peer2 = s + (2 - 4 * y) * (1 - c) + (1 - 2 * x) * c

    barrier = pltpu.get_barrier_semaphore()
    me = s * 2 + c

    def greet(d, carry):
        p = (me + d) % (2 * n)
        pl.semaphore_signal(barrier, inc=1, device_id=(p // 2, p % 2), device_id_type=MESH)
        return carry

    lax.fori_loop(1, 2 * n, greet, 0)

    part = rows // LOADS
    loads = []
    for i in range(LOADS):
        at = pl.ds(i * part, part)
        load = pltpu.make_async_copy(x_hbm.at[at], x_vm.at[at], load_sem.at[i])
        load.start()
        loads.append(load)

    def sums_of(ref, start, count, acc):
        def add(i, acc):
            at = pl.multiple_of(start + i * TILE, TILE)
            return acc + jnp.sum(ref[pl.ds(at, TILE), :].reshape(TILE // 8, 8, width), axis=0)

        return lax.fori_loop(0, count // TILE, add, acc)

    acc = jnp.zeros((8, width), jnp.float32)
    for i in range(LOADS):
        loads[i].wait()
        acc = sums_of(x_vm, i * part, part, acc)
    local_sum = jnp.sum(acc, axis=0, keepdims=True)
    sums_own[s] = local_sum
    local_mean = local_sum / rows
    mid = width // 2

    def split_own(i, carry):
        at = pl.ds(pl.multiple_of(i * TILE, TILE), TILE)
        data = x_vm[at, :] - local_mean
        hi = data.astype(jnp.bfloat16)
        lo = (data - hi.astype(jnp.float32)).astype(jnp.bfloat16)
        hi_w[at, :width] = hi
        lo_w[at, :width] = lo
        hi_w[at, width:] = hi[:, :mid]
        lo_w[at, width:] = lo[:, :mid]
        return carry

    lax.fori_loop(0, rows // TILE, split_own, 0)

    def split_other():
        acc = sums_of(other, 0, rows, jnp.zeros((8, width), jnp.float32))
        mean = jnp.sum(acc, axis=0, keepdims=True) / rows

        def body(i, carry):
            at = pl.ds(pl.multiple_of(i * TILE, TILE), TILE)
            data = other[at, :] - mean
            hi = data.astype(jnp.bfloat16)
            hi_o[at, :] = hi
            lo_o[at, :] = (data - hi.astype(jnp.float32)).astype(jnp.bfloat16)
            return carry

        lax.fori_loop(0, rows // TILE, body, 0)

    def gram(left, right):
        return lax.dot_general(
            left, right, (((0,), (0,)), ((), ())), preferred_element_type=jnp.float32
        )

    def slot_of(k):
        return c * zh + k if k < zh else (1 - c) * zh + k - zh

    def width_of(k):
        return (near if k < zh else far) * block

    def compute(k, side, dst):
        own = k < zh
        wide = width_of(k)
        hi_l, lo_l = (hi_w, lo_w) if own else (hi_o, lo_o)

        def body(b, carry):
            px = side * (1 - c) + b * c
            py = b * (1 - c) + side * c
            r = (slot_of(k) * 4 + py * 2 + px) % half
            rows_at = pl.ds(pl.multiple_of(r * block, block), block)
            start = r if own else r + c
            cols_at = pl.ds(pl.multiple_of(start * block, block), wide)
            lh, ll = hi_l[:, rows_at], lo_l[:, rows_at]
            rh, rl = hi_w[:, cols_at], lo_w[:, cols_at]
            dst[k, b, :, :wide] = gram(lh, rh) + (gram(lh, rl) + gram(ll, rh))
            return carry

        lax.fori_loop(0, 2, body, 0)

    def remote(src, dst, send, recv, scen, fac):
        return pltpu.make_async_remote_copy(
            src_ref=src, dst_ref=dst, send_sem=send, recv_sem=recv,
            device_id=(scen, fac), device_id_type=MESH,
        )

    def stage1(k):
        w = width_of(k)
        return remote(
            send1.at[k, :, :, :w], recv1.at[k, :, :, :w], s1_s.at[k], s1_r.at[k], peer1, c
        )

    def stage2(k):
        w = width_of(k)
        return remote(send2.at[k, :, :w], recv2.at[k, :, :w], s2_s.at[k], s2_r.at[k], peer2, c)

    def stage3(k):
        w = width_of(k)
        t = slot_of(k)
        place = (z - t + depth - 1) % depth
        return remote(
            zsend.at[k, :, :w], zrecv.at[place, :, :w], z_s.at[k], z_r.at[place],
            t * 4 + y * 2 + x, c,
        )

    def relay1(k):
        w = width_of(k)
        stage1(k).wait_recv()
        send2[k, :, :w] = keep1[k, 1 - second, :, :w] + recv1[k, 1 - second, :, :w]
        stage2(k).start()
        keep2[k, :, :w] = keep1[k, second, :, :w] + recv1[k, second, :, :w]

    def relay2(k):
        w = width_of(k)
        stage2(k).wait_recv()
        zsend[k, :, :w] = keep2[k, :, :w] + recv2[k, :, :w]

        @pl.when(slot_of(k) != z)
        def _():
            stage3(k).start()

    compute(0, 1 - first, send1)
    pl.semaphore_wait(barrier, 2 * n - 1)
    stage1(0).start()
    pair = remote(x_vm, other, pair_s, pair_r, s, 1 - c)
    pair.start()

    def mean_copy(d):
        p = (s + d) % n
        return remote(sums_own.at[s], sums_own.at[s], m_s.at[d], m_r.at[d], p, c)

    for d in range(1, n):
        mean_copy(d).start()

    compute(0, first, keep1)
    compute(1, 1 - first, send1)
    stage1(1).start()
    compute(1, first, keep1)

    for d in range(1, n):
        q = (s - d + n) % n
        remote(sums_own.at[q], sums_own.at[q], m_s.at[d], m_r.at[d], q, c).wait_recv()
    swap = remote(sums_own, sums_oth, mo_s, mo_r, s, 1 - c)
    swap.start()

    relay1(0)
    pair.wait_recv()
    split_other()
    compute(2, 1 - first, send1)
    stage1(2).start()
    relay1(1)
    compute(2, first, keep1)
    relay2(0)
    compute(3, 1 - first, send1)
    stage1(3).start()
    compute(3, first, keep1)
    relay2(1)

    def deviations(ref):
        sums = ref[...].reshape(n, width)
        total = jnp.sum(sums, axis=0, keepdims=True)
        return sums / rows - total / total_rows, total / total_rows

    dev, means = deviations(sums_own)
    mean_ref[...] = means
    dev_w[:, :width] = dev
    dev_w[:, width:] = dev[:, :mid]
    swap.wait_recv()
    dev_o[...] = deviations(sums_oth)[0]

    relay1(2)
    relay2(2)
    relay1(3)
    relay2(3)

    r = s % half

    def turn_copy(own, d):
        if own:
            return remote(
                turned.at[d], landed.at[d], t_s.at[d], t_r.at[d], c * half + (r + d) % half, c
            )
        return remote(
            turned.at[d], landed.at[d], t_s.at[d], t_r.at[d],
            c * half + (r + c + d) % half, 1 - c,
        )

    def finish(own):
        count = near if own else far
        w = count * block
        for k in (range(zh) if own else range(zh, 2 * zh)):
            @pl.when(slot_of(k) == z)
            def _():
                for place in range(depth - 1):
                    remote(
                        zsend.at[k, :, :w], zrecv.at[place, :, :w], z_s.at[k], z_r.at[place],
                        s, 1 - c,
                    ).wait_recv()
                left = (dev_w if own else dev_o)[:, pl.ds(pl.multiple_of(r * block, block), block)]
                start = r if own else r + c
                shift = block_gram(
                    left, dev_w[:, pl.ds(pl.multiple_of(start * block, block), w)]
                )
                value = zsend[k, :, :w]
                for place in range(depth - 1):
                    value = value + zrecv[place, :, :w]
                value = (value + rows * shift) / (total_rows - 1)
                turns = range(1, near - 1) if own else range(far)
                for d in turns:
                    turned[d] = value[:, d * block:(d + 1) * block].T
                    turn_copy(own, d).start()
                for d in range(count):
                    q = (start + d) % half
                    cov_ref[:, pl.ds(pl.multiple_of(q * block, block), block)] = value[
                        :, d * block:(d + 1) * block
                    ]
                for d in turns:
                    turn_copy(own, d).wait_recv()
                    q = (r - d + half) % half if own else (r - (1 - c) - d + 2 * half) % half
                    cov_ref[:, pl.ds(pl.multiple_of(q * block, block), block)] = landed[d]
                for d in turns:
                    turn_copy(own, d).wait_send()

    finish(True)
    finish(False)

    pair.wait_send()
    swap.wait_send()
    for d in range(1, n):
        mean_copy(d).wait_send()
    for k in range(2 * zh):
        stage1(k).wait_send()
        stage2(k).wait_send()

        @pl.when(slot_of(k) != z)
        def _():
            stage3(k).wait_send()


def by_kernel(n, scenario_pnl):
    rows, width = scenario_pnl.shape
    half = n // 2
    block = width // half
    near = half // 2 + 1
    depth = n // 4
    f32, bf16 = jnp.float32, jnp.bfloat16
    dma = pltpu.SemaphoreType.DMA
    covariance, factor_means = pl.pallas_call(
        functools.partial(kernel, n),
        out_shape=(
            jax.ShapeDtypeStruct((block, width), f32),
            jax.ShapeDtypeStruct((1, width), f32),
        ),
        in_specs=[pl.BlockSpec(memory_space=pl.ANY)],
        out_specs=[pl.BlockSpec(memory_space=pltpu.VMEM)] * 2,
        scratch_shapes=[
            pltpu.VMEM((rows, width), f32),
            pltpu.VMEM((rows, width), f32),
            pltpu.VMEM((rows, width + width // 2), bf16),
            pltpu.VMEM((rows, width + width // 2), bf16),
            pltpu.VMEM((rows, width), bf16),
            pltpu.VMEM((rows, width), bf16),
            pltpu.VMEM((depth, 2, block, near * block), f32),
            pltpu.VMEM((depth, 2, block, near * block), f32),
            pltpu.VMEM((depth, 2, block, near * block), f32),
            pltpu.VMEM((depth, block, near * block), f32),
            pltpu.VMEM((depth, block, near * block), f32),
            pltpu.VMEM((depth, block, near * block), f32),
            pltpu.VMEM((depth, block, near * block), f32),
            pltpu.VMEM((depth - 1, block, near * block), f32),
            pltpu.VMEM((near - 1, block, block), f32),
            pltpu.VMEM((near - 1, block, block), f32),
            pltpu.VMEM((n, 1, width), f32),
            pltpu.VMEM((n, 1, width), f32),
            pltpu.VMEM((n, width + width // 2), f32),
            pltpu.VMEM((n, width), f32),
            dma((LOADS,)),
            dma, dma,
            dma((depth,)), dma((depth,)),
            dma((depth,)), dma((depth,)),
            dma((depth,)), dma((depth - 1,)),
            dma((near - 1,)), dma((near - 1,)),
            dma((n,)), dma((n,)),
            dma, dma,
        ],
        compiler_params=pltpu.CompilerParams(
            collective_id=0, has_side_effects=True, vmem_limit_bytes=60 * 1024 * 1024
        ),
    )(scenario_pnl)
    return covariance, factor_means.reshape(width)


def solution(mesh):
    n, cores = mesh.shape["scen"], mesh.shape["fac"]

    def body(scenario_pnl):
        rows, width = scenario_pnl.shape
        fits = cores == 2 and n % 16 == 0 and n // 4 == 4 and width % (n * 64) == 0
        if fits and rows % (LOADS * TILE) == 0:
            return by_kernel(n, scenario_pnl)
        return on_device(scenario_pnl)

    return jax.shard_map(
        body,
        mesh=mesh,
        in_specs=(P("scen", "fac"),),
        out_specs=(P("scen", "fac"), P("fac")),
        check_vma=False,
    )
```

```python
import functools

import jax
import jax.numpy as jnp
from jax import lax
from jax.experimental import pallas as pl
from jax.experimental.pallas import tpu as pltpu
from jax.sharding import PartitionSpec as P

MESH = pl.DeviceIdType.MESH
LOADS = 4
TILE = 64


def block_gram(left, right):
    return lax.dot_general(
        left,
        right,
        (((0,), (0,)), ((), ())),
        precision=lax.Precision.HIGHEST,
        preferred_element_type=jnp.float32,
    )


def on_device(scenario_pnl):
    rows_here = scenario_pnl.shape[0]
    total_rows = rows_here * lax.axis_size("scen")
    local_sums = jnp.sum(scenario_pnl, axis=0)
    total_sums = lax.psum(local_sums, "scen")
    factor_means = total_sums / total_rows
    local_means = local_sums / rows_here
    data = scenario_pnl - local_means[None, :]
    partial_value = block_gram(lax.all_gather(data, "fac", axis=1, tiled=True), data)
    owned = lax.psum_scatter(partial_value, "scen", scatter_dimension=0, tiled=True)
    gathered = lax.all_gather(local_means, ("scen", "fac"), axis=0, tiled=True)
    spread_rows = gathered.reshape(lax.axis_size("scen"), -1)
    deviations = spread_rows - jnp.mean(spread_rows, axis=0, keepdims=True)
    owned_rows = owned.shape[0]
    column_width = owned.shape[1]
    row_part = lax.dynamic_slice_in_dim(
        deviations, lax.axis_index("scen") * owned_rows, owned_rows, 1
    )
    column_part = lax.dynamic_slice_in_dim(
        deviations, lax.axis_index("fac") * column_width, column_width, 1
    )
    owned = owned + rows_here * block_gram(row_part, column_part)
    covariance = owned / (total_rows - 1)
    return (covariance, factor_means)


def kernel(
    n, x_hbm, cov_ref, mean_ref,
    x_vm, other, hi_w, lo_w, hi_o, lo_o,
    send1, keep1, recv1, send2, recv2, zsend, zrecv,
    turned, landed, sums_own, sums_oth, dev_w, dev_o,
    load_sem, pair_s, pair_r, s1_s, s1_r, s2_s, s2_r, z_s, z_r, t_s, t_r,
    m_s, m_r, mo_s, mo_r,
):
    rows, width = x_hbm.shape
    half = n // 2
    block = width // half
    near, far = half // 2 + 1, half // 2
    depth = n // 4
    zh = depth // 2
    total_rows = rows * n

    s = lax.axis_index("scen")
    c = lax.axis_index("fac")
    z, y, x = s // 4, (s // 2) % 2, s % 2
    first = x * (1 - c) + y * c
    second = y * (1 - c) + x * c
    peer1 = s + (1 - 2 * x) * (1 - c) + (2 - 4 * y) * c
    peer2 = s + (2 - 4 * y) * (1 - c) + (1 - 2 * x) * c

    barrier = pltpu.get_barrier_semaphore()
    me = s * 2 + c

    part = rows // LOADS
    loads = []
    for i in range(LOADS):
        at = pl.ds(i * part, part)
        load = pltpu.make_async_copy(x_hbm.at[at], x_vm.at[at], load_sem.at[i])
        load.start()
        loads.append(load)

    def greet(d, carry):
        p = (me + d) % (2 * n)
        pl.semaphore_signal(barrier, inc=1, device_id=(p // 2, p % 2), device_id_type=MESH)
        return carry

    lax.fori_loop(1, 2 * n, greet, 0)

    def sums_of(ref, start, count, acc):
        def add(i, acc):
            at = pl.multiple_of(start + i * TILE, TILE)
            return acc + jnp.sum(ref[pl.ds(at, TILE), :].reshape(TILE // 8, 8, width), axis=0)

        return lax.fori_loop(0, count // TILE, add, acc)

    acc = jnp.zeros((8, width), jnp.float32)
    for i in range(LOADS):
        loads[i].wait()
        acc = sums_of(x_vm, i * part, part, acc)
    local_sum = jnp.sum(acc, axis=0, keepdims=True)
    sums_own[s] = local_sum
    local_mean = local_sum / rows
    mid = width // 2

    def split_own(i, carry):
        at = pl.ds(pl.multiple_of(i * TILE, TILE), TILE)
        data = x_vm[at, :] - local_mean
        hi = data.astype(jnp.bfloat16)
        lo = (data - hi.astype(jnp.float32)).astype(jnp.bfloat16)
        hi_w[at, :width] = hi
        lo_w[at, :width] = lo
        hi_w[at, width:] = hi[:, :mid]
        lo_w[at, width:] = lo[:, :mid]
        return carry

    lax.fori_loop(0, rows // TILE, split_own, 0)

    def split_other():
        acc = sums_of(other, 0, rows, jnp.zeros((8, width), jnp.float32))
        mean = jnp.sum(acc, axis=0, keepdims=True) / rows

        def body(i, carry):
            at = pl.ds(pl.multiple_of(i * TILE, TILE), TILE)
            data = other[at, :] - mean
            hi = data.astype(jnp.bfloat16)
            hi_o[at, :] = hi
            lo_o[at, :] = (data - hi.astype(jnp.float32)).astype(jnp.bfloat16)
            return carry

        lax.fori_loop(0, rows // TILE, body, 0)

    def gram(left, right):
        return lax.dot_general(
            left, right, (((0,), (0,)), ((), ())), preferred_element_type=jnp.float32
        )

    def slot_of(k):
        turn = (k + z) % zh
        return c * zh + turn if k < zh else (1 - c) * zh + turn

    def width_of(k):
        return (near if k < zh else far) * block

    def compute(k, side, dst, send=False):
        own = k < zh
        wide = width_of(k)
        hi_l, lo_l = (hi_w, lo_w) if own else (hi_o, lo_o)

        def body(j, carry):
            b = (1 - second) + j * (2 * second - 1)
            px = side * (1 - c) + b * c
            py = b * (1 - c) + side * c
            r = (slot_of(k) * 4 + py * 2 + px) % half
            rows_at = pl.ds(pl.multiple_of(r * block, block), block)
            start = r if own else r + c
            cols_at = pl.ds(pl.multiple_of(start * block, block), wide)
            lh, ll = hi_l[:, rows_at], lo_l[:, rows_at]
            rh, rl = hi_w[:, cols_at], lo_w[:, cols_at]
            dst[k, j, :, :wide] = gram(lh, rh) + (gram(lh, rl) + gram(ll, rh))
            if send:
                stage1(k, j).start()
            return carry

        lax.fori_loop(0, 2, body, 0)

    def remote(src, dst, send, recv, scen, fac):
        return pltpu.make_async_remote_copy(
            src_ref=src, dst_ref=dst, send_sem=send, recv_sem=recv,
            device_id=(scen, fac), device_id_type=MESH,
        )

    def stage1(k, j):
        w = width_of(k)
        return remote(
            send1.at[k, j, :, :w], recv1.at[k, j, :, :w], s1_s.at[k, j], s1_r.at[k, j], peer1, c
        )

    def stage2(k):
        w = width_of(k)
        return remote(send2.at[k, :, :w], recv2.at[k, :, :w], s2_s.at[k], s2_r.at[k], peer2, c)

    def stage3(k):
        w = width_of(k)
        t = slot_of(k)
        place = (z - t + depth - 1) % depth
        return remote(
            zsend.at[k, :, :w], zrecv.at[place, :, :w], z_s.at[k], z_r.at[place],
            t * 4 + y * 2 + x, c,
        )

    def relay1(k):
        w = width_of(k)
        stage1(k, 0).wait_recv()
        send2[k, :, :w] = keep1[k, 0, :, :w] + recv1[k, 0, :, :w]
        stage2(k).start()

    def relay2(k):
        w = width_of(k)
        stage1(k, 1).wait_recv()
        stage2(k).wait_recv()
        zsend[k, :, :w] = keep1[k, 1, :, :w] + recv1[k, 1, :, :w] + recv2[k, :, :w]

        @pl.when(slot_of(k) != z)
        def _():
            stage3(k).start()

    pl.semaphore_wait(barrier, 2 * n - 1)
    compute(0, 1 - first, send1, True)
    pair = remote(x_vm, other, pair_s, pair_r, s, 1 - c)
    pair.start()

    def mean_copy(d):
        p = (s + d) % n
        return remote(sums_own.at[s], sums_own.at[s], m_s.at[d], m_r.at[d], p, c)

    for d in range(1, n):
        mean_copy(d).start()

    compute(0, first, keep1)
    compute(1, 1 - first, send1, True)
    compute(1, first, keep1)

    for d in range(1, n):
        q = (s - d + n) % n
        remote(sums_own.at[q], sums_own.at[q], m_s.at[d], m_r.at[d], q, c).wait_recv()
    swap = remote(sums_own, sums_oth, mo_s, mo_r, s, 1 - c)
    swap.start()

    relay1(0)
    pair.wait_recv()
    split_other()
    compute(2, 1 - first, send1, True)
    relay1(1)
    compute(2, first, keep1)
    compute(3, 1 - first, send1, True)
    relay2(0)
    compute(3, first, keep1)

    def deviations(ref):
        sums = ref[...].reshape(n, width)
        total = jnp.sum(sums, axis=0, keepdims=True)
        return sums / rows - total / total_rows, total / total_rows

    dev, means = deviations(sums_own)
    mean_ref[...] = means
    dev_w[:, :width] = dev
    dev_w[:, width:] = dev[:, :mid]
    swap.wait_recv()
    dev_o[...] = deviations(sums_oth)[0]

    relay1(2)
    relay2(1)
    relay1(3)
    relay2(2)
    relay2(3)

    r = s % half

    def turn_copy(own, d):
        if own:
            return remote(
                turned.at[d], landed.at[d], t_s.at[d], t_r.at[d], c * half + (r + d) % half, c
            )
        return remote(
            turned.at[d], landed.at[d], t_s.at[d], t_r.at[d],
            c * half + (r + c + d) % half, 1 - c,
        )

    def finish(own):
        count = near if own else far
        w = count * block
        for k in (range(zh) if own else range(zh, 2 * zh)):
            @pl.when(slot_of(k) == z)
            def _():
                for place in range(depth - 1):
                    remote(
                        zsend.at[k, :, :w], zrecv.at[place, :, :w], z_s.at[k], z_r.at[place],
                        s, 1 - c,
                    ).wait_recv()
                left = (dev_w if own else dev_o)[:, pl.ds(pl.multiple_of(r * block, block), block)]
                start = r if own else r + c
                shift = block_gram(
                    left, dev_w[:, pl.ds(pl.multiple_of(start * block, block), w)]
                )
                value = zsend[k, :, :w]
                for place in range(depth - 1):
                    value = value + zrecv[place, :, :w]
                value = (value + rows * shift) / (total_rows - 1)
                turns = range(1, near - 1) if own else range(far)
                for d in turns:
                    turned[d] = value[:, d * block:(d + 1) * block].T
                    turn_copy(own, d).start()
                for d in range(count):
                    q = (start + d) % half
                    cov_ref[:, pl.ds(pl.multiple_of(q * block, block), block)] = value[
                        :, d * block:(d + 1) * block
                    ]
                for d in turns:
                    turn_copy(own, d).wait_recv()
                    q = (r - d + half) % half if own else (r - (1 - c) - d + 2 * half) % half
                    cov_ref[:, pl.ds(pl.multiple_of(q * block, block), block)] = landed[d]
                for d in turns:
                    turn_copy(own, d).wait_send()

    finish(True)
    finish(False)

    pair.wait_send()
    swap.wait_send()
    for d in range(1, n):
        mean_copy(d).wait_send()
    for k in range(2 * zh):
        stage1(k, 0).wait_send()
        stage1(k, 1).wait_send()
        stage2(k).wait_send()

        @pl.when(slot_of(k) != z)
        def _():
            stage3(k).wait_send()


def by_kernel(n, scenario_pnl):
    rows, width = scenario_pnl.shape
    half = n // 2
    block = width // half
    near = half // 2 + 1
    depth = n // 4
    f32, bf16 = jnp.float32, jnp.bfloat16
    dma = pltpu.SemaphoreType.DMA
    covariance, factor_means = pl.pallas_call(
        functools.partial(kernel, n),
        out_shape=(
            jax.ShapeDtypeStruct((block, width), f32),
            jax.ShapeDtypeStruct((1, width), f32),
        ),
        in_specs=[pl.BlockSpec(memory_space=pl.ANY)],
        out_specs=[pl.BlockSpec(memory_space=pltpu.VMEM)] * 2,
        scratch_shapes=[
            pltpu.VMEM((rows, width), f32),
            pltpu.VMEM((rows, width), f32),
            pltpu.VMEM((rows, width + width // 2), bf16),
            pltpu.VMEM((rows, width + width // 2), bf16),
            pltpu.VMEM((rows, width), bf16),
            pltpu.VMEM((rows, width), bf16),
            pltpu.VMEM((depth, 2, block, near * block), f32),
            pltpu.VMEM((depth, 2, block, near * block), f32),
            pltpu.VMEM((depth, 2, block, near * block), f32),
            pltpu.VMEM((depth, block, near * block), f32),
            pltpu.VMEM((depth, block, near * block), f32),
            pltpu.VMEM((depth, block, near * block), f32),
            pltpu.VMEM((depth - 1, block, near * block), f32),
            pltpu.VMEM((near - 1, block, block), f32),
            pltpu.VMEM((near - 1, block, block), f32),
            pltpu.VMEM((n, 1, width), f32),
            pltpu.VMEM((n, 1, width), f32),
            pltpu.VMEM((n, width + width // 2), f32),
            pltpu.VMEM((n, width), f32),
            dma((LOADS,)),
            dma, dma,
            dma((depth, 2)), dma((depth, 2)),
            dma((depth,)), dma((depth,)),
            dma((depth,)), dma((depth - 1,)),
            dma((near - 1,)), dma((near - 1,)),
            dma((n,)), dma((n,)),
            dma, dma,
        ],
        compiler_params=pltpu.CompilerParams(
            collective_id=0, has_side_effects=True, vmem_limit_bytes=60 * 1024 * 1024
        ),
    )(scenario_pnl)
    return covariance, factor_means.reshape(width)


def solution(mesh):
    n, cores = mesh.shape["scen"], mesh.shape["fac"]

    def body(scenario_pnl):
        rows, width = scenario_pnl.shape
        fits = cores == 2 and n % 16 == 0 and n // 4 == 4 and width % (n * 64) == 0
        if fits and rows % (LOADS * TILE) == 0:
            return by_kernel(n, scenario_pnl)
        return on_device(scenario_pnl)

    return jax.shard_map(
        body,
        mesh=mesh,
        in_specs=(P("scen", "fac"),),
        out_specs=(P("scen", "fac"), P("fac")),
        check_vma=False,
    )
```
